16 devices in a mesh: data: 2 (over y, z), model: 8 (over x, core).
Axes of the slice: x: 4, y: 2, z: 1, core: 2. Of those that a mesh axis runs over, the one named last changes fastest.
The devices are a block of a 4x4x8 slice.
Arguments:
- tokens: bfloat16 [16, 192, 3072], P('data'), parts along dimension 0
- seg_ids: int32 [16, 192], P('data'), parts along dimension 0
- d_out: bfloat16 [16, 192, 3072], P('data'), parts along dimension 0
- gain_attn: bfloat16 [3072], replicated
- gain_mlp: bfloat16 [3072], replicated
- w_qkv: bfloat16 [3072, 24, 3, 128], P(None, 'model')
- w_out: bfloat16 [24, 128, 3072], P('model')
- w_up: bfloat16 [3072, 8192], P(None, 'model')
- w_down: bfloat16 [8192, 3072], P('model')
Outputs:
- output 1: bfloat16 [16, 192, 3072], P('data'), parts along dimension 0
- output 2: bfloat16 [16, 192, 3072], P('data'), parts along dimension 0
- output 3: bfloat16 [6144, 24, 3, 128], P('data', 'model'), parts along dimension 0
- output 4: bfloat16 [48, 128, 3072], P(('data', 'model')), parts along dimension 0
- output 5: bfloat16 [6144, 8192], P('data', 'model'), parts along dimension 0
- output 6: bfloat16 [16384, 3072], P(('data', 'model')), parts along dimension 0
- output 7: float32 [6144], P('data'), parts along dimension 0
- output 8: float32 [6144], P('data'), parts along dimension 0
There are 2 independent parts. The reference program is written for one: setup_inputs(seed, part) draws one part's arguments, and reference() takes and returns one part's arrays. A program takes and returns all parts, laid end to end along the dimension named above; an argument that names none is the same for every part.
All inputs are finite; a program needn't handle non-finite values.
Results may differ from the reference program's by a relative error of at most 0.02.
Values are sent between devices in bfloat16 or wider.
A program may use at most 768 MiB of HBM per device.

```python
import functools
import jax
import jax.numpy as jnp
from jax import lax

SEQ_COUNT = 8
SEQ_LEN = 192
HIDDEN = 3072
HEADS = 24
HEAD_DIM = 128
FFN_DIM = 8192
NORM_EPS = 1e-5


def setup_inputs(seed: int = 0, part: int = 0) -> dict:
    part_key = jax.random.fold_in(jax.random.key(seed), part)
    key_list = jax.random.split(part_key, 3)
    shared_keys = jax.random.split(jax.random.key(seed + 1), 6)
    tokens = jax.random.normal(key_list[0], (SEQ_COUNT, SEQ_LEN, HIDDEN), jnp.float32).astype(jnp.bfloat16)
    gap_draw = jax.random.randint(key_list[1], (SEQ_COUNT, SEQ_LEN), 0, max(SEQ_LEN // 2, 1))
    positions = jnp.arange(SEQ_LEN)[None, :]
    starts = jnp.where((gap_draw == 0) & (positions > 0), 1, 0)
    seg_ids = jnp.cumsum(starts, axis=1).astype(jnp.int32)
    d_out = jax.random.normal(key_list[2], (SEQ_COUNT, SEQ_LEN, HIDDEN), jnp.float32).astype(jnp.bfloat16)
    gain_attn = (1.0 + 0.2 * jax.random.normal(shared_keys[0], (HIDDEN,), jnp.float32)).astype(jnp.bfloat16)
    gain_mlp = (1.0 + 0.2 * jax.random.normal(shared_keys[1], (HIDDEN,), jnp.float32)).astype(jnp.bfloat16)
    w_qkv = (jax.random.normal(shared_keys[2], (HIDDEN, HEADS, 3, HEAD_DIM), jnp.float32) * (1.5 * HIDDEN ** -0.5)).astype(jnp.bfloat16)
    w_out = (jax.random.normal(shared_keys[3], (HEADS, HEAD_DIM, HIDDEN), jnp.float32) * (1.5 * (HEADS * HEAD_DIM) ** -0.5)).astype(jnp.bfloat16)
    w_up = (jax.random.normal(shared_keys[4], (HIDDEN, FFN_DIM), jnp.float32) * HIDDEN ** -0.5).astype(jnp.bfloat16)
    w_down = (jax.random.normal(shared_keys[5], (FFN_DIM, HIDDEN), jnp.float32) * (1.5 * FFN_DIM ** -0.5)).astype(jnp.bfloat16)
    return {'tokens': tokens, 'seg_ids': seg_ids, 'd_out': d_out, 'gain_attn': gain_attn, 'gain_mlp': gain_mlp, 'w_qkv': w_qkv, 'w_out': w_out, 'w_up': w_up, 'w_down': w_down}


def layer_norm(values, gain_vec):
    mean_val = jnp.mean(values, axis=-1, keepdims=True)
    centered = values - mean_val
    var_val = jnp.mean(centered * centered, axis=-1, keepdims=True)
    return centered * lax.rsqrt(var_val + NORM_EPS) * gain_vec


def attend_head(head_qkv, allowed):
    scores = jnp.einsum('bqd,bkd->bqk', head_qkv[0], head_qkv[1]) * (HEAD_DIM ** -0.5)
    scores = jnp.where(allowed, scores, -1e30)
    attn_probs = jax.nn.softmax(scores, axis=-1).astype(jnp.bfloat16)
    return jnp.einsum('bqk,bkd->bqd', attn_probs.astype(jnp.float32), head_qkv[2]).astype(jnp.bfloat16)


def layer_forward(tokens, gain_attn, gain_mlp, w_qkv, w_out, w_up, w_down, allowed):
    row_count = SEQ_COUNT * SEQ_LEN
    x_f32 = tokens.astype(jnp.float32).reshape(row_count, HIDDEN)
    normed = layer_norm(x_f32, gain_attn).astype(jnp.bfloat16)
    qkv_all = jnp.dot(normed.astype(jnp.float32), w_qkv.astype(jnp.float32).reshape(HIDDEN, HEADS * 3 * HEAD_DIM), preferred_element_type=jnp.float32).astype(jnp.bfloat16)
    qkv_heads = jnp.transpose(qkv_all.astype(jnp.float32).reshape(SEQ_COUNT, SEQ_LEN, HEADS, 3, HEAD_DIM), (2, 3, 0, 1, 4))
    head_out = lax.map(jax.checkpoint(functools.partial(attend_head, allowed=allowed)), qkv_heads)
    attn_rows = jnp.transpose(head_out, (1, 2, 0, 3)).reshape(row_count, HEADS * HEAD_DIM)
    attn_proj = jnp.dot(attn_rows.astype(jnp.float32), w_out.astype(jnp.float32).reshape(HEADS * HEAD_DIM, HIDDEN), preferred_element_type=jnp.float32).astype(jnp.bfloat16)
    resid_bf = (x_f32 + attn_proj.astype(jnp.float32)).astype(jnp.bfloat16)
    resid_f32 = resid_bf.astype(jnp.float32)
    normed_mlp = layer_norm(resid_f32, gain_mlp).astype(jnp.bfloat16)
    pre_act = jnp.dot(normed_mlp.astype(jnp.float32), w_up.astype(jnp.float32), preferred_element_type=jnp.float32)
    hidden = jax.nn.gelu(pre_act, approximate=True).astype(jnp.bfloat16)
    mlp_down = jnp.dot(hidden.astype(jnp.float32), w_down.astype(jnp.float32), preferred_element_type=jnp.float32).astype(jnp.bfloat16)
    layer_out = (resid_f32 + mlp_down.astype(jnp.float32)).astype(jnp.bfloat16)
    return layer_out.reshape(SEQ_COUNT, SEQ_LEN, HIDDEN)


def reference(tokens, seg_ids, d_out, gain_attn, gain_mlp, w_qkv, w_out, w_up, w_down):
    positions = jnp.arange(SEQ_LEN)
    allowed = (seg_ids[:, :, None] == seg_ids[:, None, :]) & (positions[:, None] >= positions[None, :])[None]
    layer_fn = functools.partial(layer_forward, allowed=allowed)
    layer_out, back_fn = jax.vjp(layer_fn, tokens, gain_attn.astype(jnp.float32), gain_mlp.astype(jnp.float32), w_qkv, w_out, w_up, w_down)
    grad_list = back_fn(d_out)
    return (layer_out, grad_list[0], grad_list[3], grad_list[4], grad_list[5], grad_list[6], grad_list[1], grad_list[2])
```

```python
import functools
import jax
import jax.numpy as jnp
from jax import lax
from jax.experimental import pallas as pl
from jax.experimental.pallas import tpu as pltpu
from jax.sharding import PartitionSpec as P

NORM_EPS = 1e-5
AXIS = 'model'
F32 = jnp.float32
BF16 = jnp.bfloat16
VMEM_BYTES = 62 * 2 ** 20

MESH = pl.DeviceIdType.MESH
STEP = 48
NORM_STEP = 96
SPLIT = 2
KINDS = 18


class Ring:
    def __init__(self, part, out, own, swp, mid_a, mid_b, fin_p, fin_m, rows, load_sem, send, recv, store_sem):
        self.part, self.out, self.own, self.swp = part, out, own, swp
        self.mid_a, self.mid_b, self.fin_p, self.fin_m, self.rows = mid_a, mid_b, fin_p, fin_m, rows
        self.load_sem, self.send, self.recv, self.store_sem = load_sem, send, recv, store_sem
        me = lax.axis_index('model')
        chips = lax.axis_size('model') // 2
        chip, core = me // 2, lax.rem(me, 2)
        self.me = me
        self.peer = 2 * chip + 1 - core
        self.plus = 2 * lax.rem(chip + 1, chips) + core
        self.minus = 2 * lax.rem(chip + chips - 1, chips) + core
        self.far = 2 * lax.rem(chip + 2, chips) + core
        self.seq_len = part.shape[1]
        self.piece = self.seq_len // SPLIT
        self.half = self.piece // 2

    def barrier(self, everyone):
        sem = pltpu.get_barrier_semaphore()
        count = lax.axis_size('model')
        near = (self.peer, self.plus, self.minus)
        devices = [lax.rem(self.me + r, count) for r in range(1, count)] if everyone else near
        for dev in devices:
            pl.semaphore_signal(sem, inc=1, device_id={'model': dev}, device_id_type=MESH)
        pl.semaphore_wait(sem, len(devices))

    def rcopy(self, h, kind, src, dst, dev):
        return pltpu.make_async_remote_copy(src_ref=src, dst_ref=dst, send_sem=self.send.at[h, kind],
                                            recv_sem=self.recv.at[h, kind], device_id={'model': dev}, device_id_type=MESH)

    def p(self, h): return pl.ds(h * self.piece, self.piece)
    def a(self, h): return pl.ds(h * self.piece, self.half)
    def b(self, h): return pl.ds(h * self.piece + self.half, self.half)

    def targets(self):
        return (self.far, self.plus, self.minus, self.me)

    def swap_copy(self, h, j):
        blk = self.targets()[j]
        other = blk + 1 - 2 * lax.rem(blk, 2)
        return self.rcopy(h, j, self.part.at[other, self.p(h)], self.swp.at[j, self.p(h)], self.peer)

    def load_copy(self, h, j):
        return pltpu.make_async_copy(self.part.at[self.targets()[j], self.p(h)], self.own.at[j, self.p(h)], self.load_sem.at[h, j])

    def c4(self, h): return self.rcopy(h, 4, self.own.at[0, self.a(h)], self.mid_a.at[h], self.plus)
    def c5(self, h): return self.rcopy(h, 5, self.own.at[0, self.b(h)], self.mid_b.at[h], self.minus)
    def c6(self, h): return self.rcopy(h, 6, self.own.at[1, self.b(h)], self.fin_p.at[self.b(h)], self.plus)
    def c7(self, h): return self.rcopy(h, 7, self.own.at[2, self.a(h)], self.fin_m.at[self.a(h)], self.minus)
    def c8(self, h): return self.rcopy(h, 8, self.own.at[1, self.a(h)], self.fin_p.at[self.a(h)], self.plus)
    def c9(self, h): return self.rcopy(h, 9, self.own.at[2, self.b(h)], self.fin_m.at[self.b(h)], self.minus)
    def c10(self, h): return self.rcopy(h, 10, self.rows.at[self.p(h)], self.out.at[self.me, self.p(h)], self.plus)
    def c11(self, h): return self.rcopy(h, 11, self.rows.at[self.p(h)], self.out.at[self.me, self.p(h)], self.minus)
    def c12(self, h): return self.rcopy(h, 12, self.rows.at[self.p(h)], self.out.at[self.me, self.p(h)], self.peer)
    def c13(self, h): return self.rcopy(h, 13, self.out.at[self.minus, self.a(h)], self.out.at[self.minus, self.a(h)], self.plus)
    def c14(self, h): return self.rcopy(h, 14, self.out.at[self.plus, self.b(h)], self.out.at[self.plus, self.b(h)], self.minus)
    def c15(self, h): return self.rcopy(h, 15, self.out.at[self.minus, self.p(h)], self.out.at[self.minus, self.p(h)], self.peer)
    def c16(self, h): return self.rcopy(h, 16, self.out.at[self.plus, self.p(h)], self.out.at[self.plus, self.p(h)], self.peer)
    def c17(self, h): return self.rcopy(h, 17, self.out.at[self.far, self.p(h)], self.out.at[self.far, self.p(h)], self.peer)
    def keep(self, h): return pltpu.make_async_copy(self.rows.at[self.p(h)], self.out.at[self.me, self.p(h)], self.store_sem.at[h])

    def begin(self, everyone=False):
        for h in range(SPLIT):
            for j in range(4):
                self.load_copy(h, j).start()
        self.barrier(everyone)
        for h in range(SPLIT):
            for j in range(4):
                self.swap_copy(h, j).start()

    def add(self, j, row0, count, src, src_row0):
        def body(i, carry):
            at = pl.ds(pl.multiple_of(row0 + i * STEP, STEP), STEP)
            fr = pl.ds(pl.multiple_of(src_row0 + i * STEP, STEP), STEP)
            self.own[j, at] = (self.own[j, at].astype(jnp.float32) + src[fr].astype(jnp.float32)).astype(jnp.bfloat16)
            return carry
        lax.fori_loop(0, count // STEP, body, 0)

    def merge_swap(self, h, j):
        self.load_copy(h, j).wait()
        self.swap_copy(h, j).wait_recv()
        self.add(j, h * self.piece, self.piece, self.swp.at[j], h * self.piece)

    def first(self, h):
        self.merge_swap(h, 0)
        self.c4(h).start()
        self.c5(h).start()
        self.merge_swap(h, 1)
        self.c6(h).start()
        self.merge_swap(h, 2)
        self.c7(h).start()

    def second(self, h):
        self.c4(h).wait_recv()
        self.add(1, h * self.piece, self.half, self.mid_a.at[h], 0)
        self.c8(h).start()
        self.c5(h).wait_recv()
        self.add(2, h * self.piece + self.half, self.half, self.mid_b.at[h], 0)
        self.c9(h).start()

    def finish(self, h, middle):
        self.load_copy(h, 3).wait()
        self.swap_copy(h, 3).wait_recv()
        self.c6(h).wait_recv()
        self.c8(h).wait_recv()
        self.c7(h).wait_recv()
        self.c9(h).wait_recv()

        def body(i, carry):
            at = pl.ds(pl.multiple_of(h * self.piece + i * STEP, STEP), STEP)
            f = lambda r: r.astype(jnp.float32)
            total = (f(self.own[3, at]) + f(self.swp[3, at])) + (f(self.fin_p[at]) + f(self.fin_m[at]))
            return middle(at, total, carry)
        return lax.fori_loop(0, self.piece // STEP, body, 0)

    def share(self, h):
        self.keep(h).start()
        self.c10(h).start()
        self.c11(h).start()
        self.c12(h).start()

    def forward(self, h):
        self.c10(h).wait_recv()
        self.c13(h).start()
        self.c15(h).start()
        self.c11(h).wait_recv()
        self.c14(h).start()
        self.c16(h).start()

    def last(self, h):
        self.c13(h).wait_recv()
        self.c14(h).wait_recv()
        self.c17(h).start()

    def end(self):
        for h in range(SPLIT):
            for c in (self.c12, self.c15, self.c16, self.c17):
                c(h).wait_recv()
            for j in range(4):
                self.swap_copy(h, j).wait_send()
            for c in (self.c4, self.c5, self.c6, self.c7, self.c8, self.c9, self.c10, self.c11, self.c12, self.c13, self.c14, self.c15, self.c16, self.c17):
                c(h).wait_send()
            self.keep(h).wait()


def ring_scratch(seq_len, hidden):
    bf = jnp.bfloat16
    return [pltpu.VMEM((4, seq_len, hidden), bf), pltpu.VMEM((4, seq_len, hidden), bf),
            pltpu.VMEM((SPLIT, seq_len // SPLIT // 2, hidden), bf), pltpu.VMEM((SPLIT, seq_len // SPLIT // 2, hidden), bf),
            pltpu.VMEM((seq_len, hidden), bf), pltpu.VMEM((seq_len, hidden), bf), pltpu.VMEM((seq_len, hidden), bf),
            pltpu.SemaphoreType.DMA((SPLIT, 4)), pltpu.SemaphoreType.DMA((SPLIT, KINDS)), pltpu.SemaphoreType.DMA((SPLIT, KINDS)),
            pltpu.SemaphoreType.DMA((SPLIT,))]


def any_spec():
    return pl.BlockSpec(memory_space=pl.ANY)


def dot_nn(lhs, rhs):
    return lax.dot_general(lhs, rhs, (((1,), (0,)), ((), ())), preferred_element_type=F32)


def dot_nt(lhs, rhs):
    return lax.dot_general(lhs, rhs, (((1,), (1,)), ((), ())), preferred_element_type=F32)


def dot_tn(lhs, rhs):
    return lax.dot_general(lhs, rhs, (((0,), (0,)), ((), ())), preferred_element_type=F32)


def norm_stats(values):
    mean_val = jnp.mean(values, axis=-1, keepdims=True)
    centered = values - mean_val
    var_val = jnp.mean(centered * centered, axis=-1, keepdims=True)
    return centered, lax.rsqrt(var_val + NORM_EPS)


def norm_back(values, gain, grad):
    centered, scale = norm_stats(values)
    unit = centered * scale
    d_unit = grad * gain
    mean_d = jnp.mean(d_unit, axis=-1, keepdims=True)
    mean_du = jnp.mean(d_unit * unit, axis=-1, keepdims=True)
    return scale * (d_unit - mean_d - unit * mean_du), grad * unit


def softmax_of(q, k, keep):
    scores = dot_nt(q, k) * (q.shape[-1] ** -0.5)
    scores = jnp.where(keep > 0.5, scores, -1e30)
    top = jnp.max(scores, axis=-1, keepdims=True)
    weights = jnp.exp(scores - top)
    return weights / jnp.sum(weights, axis=-1, keepdims=True)


def columns_dot(dot, out, lhs, rhs_of, width):
    for c in range(out.shape[-1] // width):
        out[:, c * width:(c + 1) * width] = dot(lhs, rhs_of(c * width, width)).astype(BF16)


def attention_seq(x, a, qkv, o, p1, keep, gain, wq, wo):
    def norm_step(i, carry):
        at = pl.ds(pl.multiple_of(i * NORM_STEP, NORM_STEP), NORM_STEP)
        centered, scale = norm_stats(x[at].astype(F32))
        a[at] = (centered * scale * gain[...]).astype(BF16)
        return carry
    lax.fori_loop(0, x.shape[0] // NORM_STEP, norm_step, 0)
    dim = 128
    for n in range(o.shape[-1] // dim):
        lo = 3 * n * dim
        qkv[:, lo:lo + 3 * dim] = dot_nn(a[...], wq[:, lo:lo + 3 * dim]).astype(BF16)
        q, k, v = (qkv[:, lo + j * dim:lo + (j + 1) * dim] for j in range(3))
        probs = softmax_of(q, k, keep[...]).astype(BF16)
        o[:, n * dim:(n + 1) * dim] = dot_nn(probs, v).astype(BF16)
    columns_dot(dot_nn, p1, o[...], lambda c, w: wo[:, c:c + w], 768)


def attention_back_seq(d_x1, qkv, keep, wq, wo, d_qkv, d_a):
    heads_width = wo.shape[0]
    dim = 128
    d_heads = dot_nt(d_x1[...], wo[...]).astype(BF16)
    for n in range(heads_width // dim):
        lo = 3 * n * dim
        q, k, v = (qkv[:, lo + j * dim:lo + (j + 1) * dim] for j in range(3))
        d_o = d_heads[:, n * dim:(n + 1) * dim]
        probs = softmax_of(q, k, keep[...])
        d_probs = dot_nt(d_o, v)
        row_dot = jnp.sum(d_probs * probs, axis=-1, keepdims=True)
        d_scores = (probs * (d_probs - row_dot) * (dim ** -0.5)).astype(BF16)
        d_qkv[:, lo:lo + dim] = dot_nn(d_scores, k).astype(BF16)
        d_qkv[:, lo + dim:lo + 2 * dim] = dot_tn(d_scores, q).astype(BF16)
        d_qkv[:, lo + 2 * dim:lo + 3 * dim] = dot_tn(probs.astype(BF16), d_o).astype(BF16)
    columns_dot(dot_nt, d_a, d_qkv[...], lambda c, w: wq[c:c + w, :], 512)


def load_wq(wq_hbm, wq, sems):
    dim = wq_hbm.shape[-1]
    return [pltpu.make_async_copy(wq_hbm.at[i], wq.at[:, pl.ds(i * dim, dim)], sems.at[i]) for i in range(wq_hbm.shape[0])]


class Stream:
    def __init__(self, count, in_pairs, out_pairs, in_sem, out_sem):
        self.count, self.in_pairs, self.out_pairs, self.in_sem, self.out_sem = count, in_pairs, out_pairs, in_sem, out_sem

    def loads(self, i, slot):
        return [pltpu.make_async_copy(a, b, self.in_sem.at[k, slot]) for k, (a, b) in enumerate(self.in_pairs(i, slot))]

    def stores(self, i, slot):
        return [pltpu.make_async_copy(a, b, self.out_sem.at[k, slot]) for k, (a, b) in enumerate(self.out_pairs(i, slot))]

    def begin(self):
        for c in self.loads(0, 0):
            c.start()

    def run(self, lo, hi, body):
        def step(i, carry):
            slot = lax.rem(i, 2)
            for c in self.loads(i, slot):
                c.wait()

            @pl.when(i + 1 < self.count)
            def _():
                for c in self.loads(i + 1, 1 - slot):
                    c.start()

            @pl.when(i >= 2)
            def _():
                for c in self.stores(i - 2, slot):
                    c.wait()
            body(slot)
            for c in self.stores(i, slot):
                c.start()
            return carry
        lax.fori_loop(lo, hi, step, 0)

    def end(self):
        for i in (self.count - 2, self.count - 1):
            for c in self.stores(i, i % 2):
                c.wait()


def ring_params(cid):
    return pltpu.CompilerParams(collective_id=cid, has_side_effects=True, vmem_limit_bytes=VMEM_BYTES)


def sds(shape, dtype=BF16):
    return jax.ShapeDtypeStruct(shape, dtype)


def first_kernel(x, keep, gain, wq_hbm, wo, p1, wq, a, qkv, o, sems):
    @pl.when(pl.program_id(0) == 0)
    def _():
        copies = load_wq(wq_hbm, wq, sems)
        for c in copies:
            c.start()
        for c in copies:
            c.wait()
    attention_seq(x.at[0], a, qkv, o, p1.at[0], keep.at[0], gain, wq, wo)


def first_call(tokens, keep, gain, wq, wo):
    seqs, seq_len, hidden = tokens.shape
    width = wq.shape[0] * wq.shape[2]
    seq = lambda w: pl.BlockSpec((1, seq_len, w), lambda i: (i, 0, 0))
    return pl.pallas_call(
        first_kernel, grid=(seqs,), out_shape=sds(tokens.shape),
        in_specs=[seq(hidden), seq(seq_len), pl.BlockSpec(gain.shape, lambda i: (0, 0)), any_spec(), pl.BlockSpec(wo.shape, lambda i: (0, 0))],
        out_specs=seq(hidden),
        scratch_shapes=[pltpu.VMEM((hidden, width), BF16), pltpu.VMEM((seq_len, hidden), BF16), pltpu.VMEM((seq_len, width), BF16),
                        pltpu.VMEM((seq_len, wo.shape[0]), BF16), pltpu.SemaphoreType.DMA((wq.shape[0],))],
        compiler_params=pltpu.CompilerParams(vmem_limit_bytes=VMEM_BYTES),
        cost_estimate=pl.CostEstimate(flops=20 * 10 ** 9, bytes_accessed=30 * 10 ** 6, transcendentals=0))(tokens, keep, gain, wq, wo)


def residual_events(ring, x_rows, x1_rows, gain):
    def middle(at, total, carry):
        x1 = (x_rows[at].astype(F32) + total.astype(BF16).astype(F32)).astype(BF16)
        x1_rows[at] = x1
        centered, scale = norm_stats(x1.astype(F32))
        ring.rows[at] = (centered * scale * gain[...]).astype(BF16)
        return carry
    return ring_events(ring, middle)


def ring_events(ring, middle):
    events = [functools.partial(ring.first, h) for h in range(SPLIT)]
    events += [functools.partial(ring.second, h) for h in range(SPLIT)]

    def close(h):
        ring.finish(h, middle)
        ring.share(h)
    events += [functools.partial(close, h) for h in range(SPLIT)]
    events += [functools.partial(ring.forward, h) for h in range(SPLIT)]
    events += [functools.partial(ring.last, h) for h in range(SPLIT)]
    return events


def interleave(events, tasks, counts):
    pending = [[run, 0, total] for total, run in tasks]
    for event, n in zip(events, counts):
        while n and pending:
            run, lo, total = pending[0]
            hi = min(lo + n, total)
            run(lo, hi)
            n -= hi - lo
            pending[0][1] = hi
            if hi == total:
                pending.pop(0)
        event()
    for run, lo, total in pending:
        run(lo, total)


def ka_kernel(p1, tokens, keep, gain_a, gain_m, wq_hbm, wo_hbm,
              b_out, x1_out, a_out, qkv_out, o_out, p1_out,
              x_rows, x1_rows, row_sem, wq, wo, wq_sem, wo_sem, x2, keep2, a2, qkv2, o2, p2, in_sem, out_sem, *ring_scr):
    ring = Ring(p1, b_out, *ring_scr)
    ring.begin()
    loads = [pltpu.make_async_copy(tokens.at[ring.me], x_rows, row_sem.at[0]), pltpu.make_async_copy(wo_hbm, wo, wo_sem)]
    weights = load_wq(wq_hbm, wq, wq_sem)
    stream = Stream(tokens.shape[0], lambda i, t: [(tokens.at[i], x2.at[t]), (keep.at[i], keep2.at[t])],
                    lambda i, t: [(a2.at[t], a_out.at[i]), (qkv2.at[t], qkv_out.at[i]), (o2.at[t], o_out.at[i]), (p2.at[t], p1_out.at[i])],
                    in_sem, out_sem)
    for c in loads + weights:
        c.start()
    stream.begin()
    for c in loads + weights:
        c.wait()

    def task(lo, hi):
        stream.run(lo, hi, lambda t: attention_seq(x2.at[t], a2.at[t], qkv2.at[t], o2.at[t], p2.at[t], keep2.at[t], gain_a, wq, wo))
    interleave(residual_events(ring, x_rows, x1_rows, gain_m), [(stream.count, task)], PLAN)
    keep_rows = pltpu.make_async_copy(x1_rows, x1_out, row_sem.at[1])
    keep_rows.start()
    stream.end()
    keep_rows.wait()
    ring.end()


PLAN = (0, 0, 1, 2, 2, 1, 1, 1, 0, 0)


def ka_call(p1, tokens, keep, gain_a, gain_m, wq, wo, cid):
    seqs, seq_len, hidden = tokens.shape
    width, inner = wq.shape[0] * wq.shape[2], wo.shape[0]
    vm = pl.BlockSpec(memory_space=pltpu.VMEM)
    two = lambda w, t=BF16: pltpu.VMEM((2, seq_len, w), t)
    full = lambda w: sds((seqs, seq_len, w))
    return pl.pallas_call(
        ka_kernel, out_shape=(full(hidden), sds((seq_len, hidden)), full(hidden), full(width), full(inner), full(hidden)),
        in_specs=[any_spec()] * 3 + [vm, vm] + [any_spec()] * 2, out_specs=(any_spec(),) * 6,
        scratch_shapes=[pltpu.VMEM((seq_len, hidden), BF16), pltpu.VMEM((seq_len, hidden), BF16), pltpu.SemaphoreType.DMA((2,)),
                        pltpu.VMEM((hidden, width), BF16), pltpu.VMEM((inner, hidden), BF16), pltpu.SemaphoreType.DMA((wq.shape[0],)), pltpu.SemaphoreType.DMA,
                        two(hidden), two(seq_len, F32), two(hidden), two(width), two(inner), two(hidden),
                        pltpu.SemaphoreType.DMA((2, 2)), pltpu.SemaphoreType.DMA((4, 2))] + ring_scratch(seq_len, hidden),
        compiler_params=ring_params(cid),
        cost_estimate=pl.CostEstimate(flops=80 * 10 ** 9, bytes_accessed=80 * 10 ** 6, transcendentals=0))(p1, tokens, keep, gain_a, gain_m, wq, wo)


def gelu(values):
    return jax.nn.gelu(values, approximate=True)


def mlp_seq(b, p2, hid, w_up, w_down):
    inner = w_up.shape[1]
    for c in range(0, inner, 256):
        hid[:, c:c + 256] = gelu(dot_nn(b[...], w_up[:, c:c + 256])).astype(BF16)
    columns_dot(dot_nn, p2, hid[...], lambda c, w: w_down[:, c:c + w], 512)


def kb_kernel(p1, tokens, b_fwd, gain_m, up_hbm, down_hbm, b_out, x1_out, p2_out,
              x_rows, x1_rows, row_sem, w_up, w_down, w_sem, b2, p2, hid, in_sem, out_sem, *ring_scr):
    ring = Ring(p1, b_out, *ring_scr)
    ring.begin()
    loads = [pltpu.make_async_copy(tokens.at[ring.me], x_rows, row_sem.at[0]),
             pltpu.make_async_copy(up_hbm, w_up, w_sem.at[0]), pltpu.make_async_copy(down_hbm, w_down, w_sem.at[1])]
    stream = Stream(b_fwd.shape[0], lambda i, t: [(b_fwd.at[i], b2.at[t])], lambda i, t: [(p2.at[t], p2_out.at[i])], in_sem, out_sem)
    for c in loads:
        c.start()
    stream.begin()
    for c in loads:
        c.wait()

    def task(lo, hi):
        stream.run(lo, hi, lambda t: mlp_seq(b2.at[t], p2.at[t], hid, w_up, w_down))
    interleave(residual_events(ring, x_rows, x1_rows, gain_m), [(stream.count, task)], PLAN)
    keep_rows = pltpu.make_async_copy(x1_rows, x1_out, row_sem.at[1])
    keep_rows.start()
    stream.end()
    keep_rows.wait()
    ring.end()


def kb_call(p1, tokens, b_fwd, gain_m, w_up, w_down, cid):
    seqs, seq_len, hidden = tokens.shape
    inner = w_up.shape[1]
    vm = pl.BlockSpec(memory_space=pltpu.VMEM)
    return pl.pallas_call(
        kb_kernel, out_shape=(sds(tokens.shape), sds((seq_len, hidden)), sds(tokens.shape)),
        in_specs=[any_spec()] * 3 + [vm] + [any_spec()] * 2, out_specs=(any_spec(),) * 3,
        scratch_shapes=[pltpu.VMEM((seq_len, hidden), BF16), pltpu.VMEM((seq_len, hidden), BF16), pltpu.SemaphoreType.DMA((2,)),
                        pltpu.VMEM((hidden, inner), BF16), pltpu.VMEM((inner, hidden), BF16), pltpu.SemaphoreType.DMA((2,)),
                        pltpu.VMEM((2, seq_len, hidden), BF16), pltpu.VMEM((2, seq_len, hidden), BF16), pltpu.VMEM((seq_len, inner), BF16),
                        pltpu.SemaphoreType.DMA((1, 2)), pltpu.SemaphoreType.DMA((1, 2))] + ring_scratch(seq_len, hidden),
        compiler_params=ring_params(cid),
        cost_estimate=pl.CostEstimate(flops=80 * 10 ** 9, bytes_accessed=80 * 10 ** 6, transcendentals=0))(p1, tokens, b_fwd, gain_m, w_up, w_down)


TILE = 384
NARROW = 128
GRAD_PLAN = (0, 0, 2, 4, 4, 2, 2, 2, 0, 0)


def wide_task(lhs_hbm, rhs, out_pairs, l2, g2, sems):
    in_sem, out_sem = sems
    stream = Stream(lhs_hbm.shape[1] // TILE, lambda i, t: [(lhs_hbm.at[:, pl.ds(pl.multiple_of(i * TILE, TILE), TILE)], l2.at[t])], out_pairs, in_sem, out_sem)

    def run(lo, hi):
        stream.run(lo, hi, lambda t: g2.__setitem__(t, dot_tn(l2[t], rhs[...]).astype(BF16)))
    return stream, run


def narrow_task(lhs_hbm, rhs, out_hbm, l2, g2, sems):
    in_sem, out_sem = sems
    span = lambda i: pl.ds(pl.multiple_of(i * NARROW, NARROW), NARROW)
    stream = Stream(lhs_hbm.shape[1] // NARROW, lambda i, t: [(lhs_hbm.at[:, span(i)], l2.at[t])], lambda i, t: [(g2.at[t], out_hbm.at[span(i)])], in_sem, out_sem)

    def run(lo, hi):
        def body(t):
            lhs = l2[t]
            for c in range(0, rhs.shape[1], 1024):
                g2[t, :, c:c + 1024] = dot_tn(lhs, rhs[:, c:c + 1024]).astype(BF16)
        stream.run(lo, hi, body)
    return stream, run


def grad_kernel(last, part, values, resid, gain, wide_l, wide_r, narrow_l, narrow_r, *refs):
    if last:
        other_gain, out, gains_out, wide_out, narrow_out = refs[:5]
        refs = refs[5:]
    else:
        out, gain_out, wide_out, narrow_out = refs[:4]
        refs = refs[4:]
    v_rows, r_rows, row_sem, d_gain, w_r, w_l2, w_g2, n_r, n_l2, n_g2, rhs_sem, w_in, w_outs, n_in, n_outs = refs[:15]
    refs = refs[15:]
    if last:
        g_send, g_recv, g_ssem, g_rsem = refs[:4]
        refs = refs[4:]
    ring = Ring(part, out, *refs)
    ring.begin(everyone=last)
    loads = [pltpu.make_async_copy(values.at[ring.me] if len(values.shape) == 3 else values, v_rows, row_sem.at[0]),
             pltpu.make_async_copy(resid.at[ring.me], r_rows, row_sem.at[1]),
             pltpu.make_async_copy(wide_r, w_r, rhs_sem.at[0]), pltpu.make_async_copy(narrow_r, n_r, rhs_sem.at[1])]
    for c in loads:
        c.start()

    def wide_pairs(i, t):
        at = pl.ds(pl.multiple_of(i * TILE, TILE), TILE)
        if len(wide_out.shape) == 2:
            return [(w_g2.at[t], wide_out.at[at])]
        dim = wide_out.shape[2]
        return [(w_g2.at[t, :, pl.ds(j * dim, dim)], wide_out.at[j, at]) for j in range(wide_out.shape[0])]
    wide, wide_run = wide_task(wide_l, w_r, wide_pairs, w_l2, w_g2, (w_in, w_outs))
    narrow, narrow_run = narrow_task(narrow_l, n_r, narrow_out, n_l2, n_g2, (n_in, n_outs))
    wide.begin()
    narrow.begin()
    for c in loads:
        c.wait()

    d_gain[...] = jnp.zeros_like(d_gain)

    def middle(at, total, carry):
        d_value, d_gain_part = norm_back(v_rows[at].astype(F32), gain[...], total.astype(BF16).astype(F32))
        ring.rows[at] = (r_rows[at].astype(F32) + d_value).astype(BF16)
        d_gain[...] += d_gain_part
        return carry
    events = ring_events(ring, middle)
    hidden = part.shape[2]
    count = lax.axis_size(AXIS)

    def gain_copy(r, sender):
        target = lax.rem(ring.me + r, count)
        return pltpu.make_async_remote_copy(src_ref=g_send, dst_ref=g_recv.at[sender], send_sem=g_ssem.at[r], recv_sem=g_rsem.at[sender],
                                            device_id={AXIS: target}, device_id_type=MESH)

    def gains():
        mine = jnp.sum(d_gain[...], axis=0, keepdims=True)
        if not last:
            gain_out[...] = mine
            return
        g_send[:, :hidden] = mine
        g_send[:, hidden:] = other_gain[...]
        g_recv[ring.me, :, :hidden] = mine
        g_recv[ring.me, :, hidden:] = other_gain[...]
        for r in range(1, count):
            gain_copy(r, ring.me).start()
    events.insert(2 * SPLIT + SPLIT, gains)
    plan = GRAD_PLAN[:3 * SPLIT] + (0,) + GRAD_PLAN[3 * SPLIT:]
    interleave(events, [(wide.count, wide_run), (narrow.count, narrow_run)], plan)
    wide.end()
    narrow.end()
    ring.end()
    if last:
        for r in range(1, count):
            gain_copy(r, lax.rem(ring.me + r, count)).wait_recv()
            gain_copy(r, ring.me).wait_send()
        total = g_recv[0]
        for r in range(1, count):
            total = total + g_recv[r]
        gains_out[...] = total


def grad_call(part, values, resid, gain, wide_l, wide_r, narrow_l, narrow_r, blocks, cid, other_gain=None):
    seqs, seq_len, hidden = part.shape
    last = other_gain is not None
    vm = pl.BlockSpec(memory_space=pltpu.VMEM)
    rows, wide_n, narrow_n = wide_r.shape[0], wide_r.shape[1], narrow_r.shape[1]
    wide_shape = (wide_l.shape[1], wide_n) if blocks == 1 else (blocks, wide_l.shape[1], wide_n // blocks)
    dma = pltpu.SemaphoreType.DMA
    outs = (sds(part.shape), sds((1, 2 * hidden if last else hidden), F32), sds(wide_shape), sds((narrow_l.shape[1], narrow_n)))
    scratch = [pltpu.VMEM((seq_len, hidden), BF16), pltpu.VMEM((seq_len, hidden), BF16), dma((2,)), pltpu.VMEM((STEP, hidden), F32),
               pltpu.VMEM((rows, wide_n), BF16), pltpu.VMEM((2, rows, TILE), BF16), pltpu.VMEM((2, TILE, wide_n), BF16),
               pltpu.VMEM((rows, narrow_n), BF16), pltpu.VMEM((2, rows, NARROW), BF16), pltpu.VMEM((2, NARROW, narrow_n), BF16),
               dma((2,)), dma((1, 2)), dma((blocks, 2)), dma((1, 2)), dma((1, 2))]
    if last:
        count = lax.axis_size(AXIS)
        scratch += [pltpu.VMEM((1, 2 * hidden), F32), pltpu.VMEM((count, 1, 2 * hidden), F32), dma((count,)), dma((count,))]
    args = (part, values, resid, gain, wide_l, wide_r, narrow_l, narrow_r) + ((other_gain,) if last else ())
    return pl.pallas_call(
        functools.partial(grad_kernel, last), out_shape=outs,
        in_specs=[any_spec()] * 3 + [vm] + [any_spec()] * 4 + ([vm] if last else []), out_specs=(any_spec(), vm, any_spec(), any_spec()),
        scratch_shapes=scratch + ring_scratch(seq_len, hidden), compiler_params=ring_params(cid),
        cost_estimate=pl.CostEstimate(flops=80 * 10 ** 9, bytes_accessed=80 * 10 ** 6, transcendentals=0))(*args)


def back_kernel(d_x1, qkv, keep, wq_hbm, wo, d_qkv, d_a, wq, sems):
    @pl.when(pl.program_id(0) == 0)
    def _():
        copies = load_wq(wq_hbm, wq, sems)
        for c in copies:
            c.start()
        for c in copies:
            c.wait()
    attention_back_seq(d_x1.at[0], qkv.at[0], keep.at[0], wq, wo, d_qkv.at[0], d_a.at[0])


def back_call(d_x1, qkv, keep, wq, wo):
    seqs, seq_len, hidden = d_x1.shape
    width = qkv.shape[-1]
    seq = lambda w: pl.BlockSpec((1, seq_len, w), lambda i: (i, 0, 0))
    return pl.pallas_call(
        back_kernel, grid=(seqs,), out_shape=(sds(qkv.shape), sds(d_x1.shape)),
        in_specs=[seq(hidden), seq(width), seq(seq_len), any_spec(), pl.BlockSpec(wo.shape, lambda i: (0, 0))],
        out_specs=(seq(width), seq(hidden)),
        scratch_shapes=[pltpu.VMEM((hidden, width), BF16), pltpu.SemaphoreType.DMA((wq.shape[0],))],
        compiler_params=pltpu.CompilerParams(vmem_limit_bytes=VMEM_BYTES),
        cost_estimate=pl.CostEstimate(flops=20 * 10 ** 9, bytes_accessed=30 * 10 ** 6, transcendentals=0))(d_x1, qkv, keep, wq, wo)


def dot_of(spec, lhs, rhs):
    return jnp.einsum(spec, lhs, rhs, preferred_element_type=F32)


def solution(mesh):
    def device_step(tokens, seg_ids, d_out, gain_attn, gain_mlp, w_qkv, w_out, w_up, w_down):
        seqs, seq_len, hidden = tokens.shape
        row_count = seqs * seq_len
        heads, dim = w_qkv.shape[1], w_qkv.shape[3]
        at_pos = lax.broadcasted_iota(jnp.int32, (seq_len, seq_len), 0) >= lax.broadcasted_iota(jnp.int32, (seq_len, seq_len), 1)
        keep = ((seg_ids[:, :, None] == seg_ids[:, None, :]) & at_pos[None]).astype(F32)
        gain_a = gain_attn.astype(F32)[None]
        gain_m = gain_mlp.astype(F32)[None]
        wq = jnp.transpose(w_qkv, (1, 2, 0, 3)).reshape(heads * 3, hidden, dim)
        wo = w_out.reshape(heads * dim, hidden)
        flat = lambda v: v.reshape(row_count, v.shape[-1])

        p1 = first_call(tokens, keep, gain_a, wq, wo)
        b_full, x1_rows, normed, qkv, heads_out, p1_again = ka_call(p1, tokens, keep, gain_a, gain_m, wq, wo, 0)
        b_again, x1_again, p2 = kb_call(p1_again, tokens, b_full, gain_m, w_up, w_down, 1)
        p2_rows = lax.psum_scatter(flat(p2), AXIS, scatter_dimension=0, tiled=True)
        out_rows = (x1_rows.astype(F32) + p2_rows.astype(F32)).astype(BF16)

        pre_act = dot_of('rh,hf->rf', flat(b_again), w_up)
        hidden_act, gelu_back = jax.vjp(gelu, pre_act)
        hidden_act = hidden_act.astype(BF16)
        d_hidden = dot_of('rh,fh->rf', flat(d_out), w_down).astype(BF16)
        d_pre = gelu_back(d_hidden.astype(F32))[0].astype(BF16)
        d_b = dot_of('rf,hf->rh', d_pre, w_up).astype(BF16).reshape(tokens.shape)
        d_x1, d_gain_m, d_w_up, d_w_down = grad_call(d_b, x1_again, d_out, gain_m, flat(b_again), d_pre, hidden_act, flat(d_out), 1, 2)
        d_x1, out_rows = lax.optimization_barrier((d_x1, out_rows))
        layer_out = lax.all_gather(out_rows, AXIS, axis=0, tiled=True).reshape(tokens.shape)
        d_qkv, d_a = back_call(d_x1, qkv, keep, wq, wo)
        d_tokens, d_gain, d_wq, d_wo = grad_call(d_a, tokens, d_x1, gain_a, flat(normed), flat(d_qkv), flat(heads_out), flat(d_x1), heads * 3, 3, d_gain_m)
        d_w_qkv = jnp.transpose(d_wq.reshape(heads, 3, hidden, dim), (2, 0, 1, 3))
        d_w_out = d_wo.reshape(w_out.shape)
        d_gain_a, d_gain_m = d_gain[0, :hidden], d_gain[0, hidden:]
        return layer_out, d_tokens, d_w_qkv, d_w_out, d_w_up, d_w_down, d_gain_a, d_gain_m

    in_specs = (P('data', None, None), P('data', None), P('data', None, None), P(), P(), P(None, 'model', None, None), P('model', None, None), P(None, 'model'), P('model', None))
    out_specs = (P('data', None, None), P('data', None, None), P('data', 'model', None, None), P(('data', 'model'), None, None), P('data', 'model'), P(('data', 'model'), None), P('data'), P('data'))
    return jax.shard_map(device_step, mesh=mesh, in_specs=in_specs, out_specs=out_specs, check_vma=False)
```

```python
import functools
import jax
import jax.numpy as jnp
from jax import lax
from jax.experimental import pallas as pl
from jax.experimental.pallas import tpu as pltpu
from jax.sharding import PartitionSpec as P

NORM_EPS = 1e-5
AXIS = 'model'
F32 = jnp.float32
BF16 = jnp.bfloat16
VMEM_BYTES = 62 * 2 ** 20

MESH = pl.DeviceIdType.MESH
STEP = 48
NORM_STEP = 96
SPLIT = 2
KINDS = 18


class Ring:
    def __init__(self, part, out, own, swp, mid_a, mid_b, fin_p, fin_m, rows, load_sem, send, recv, store_sem, give=None):
        self.part, self.out, self.own, self.swp, self.give = part, out, own, swp, give
        self.mid_a, self.mid_b, self.fin_p, self.fin_m, self.rows = mid_a, mid_b, fin_p, fin_m, rows
        self.load_sem, self.send, self.recv, self.store_sem = load_sem, send, recv, store_sem
        me = lax.axis_index('model')
        chips = lax.axis_size('model') // 2
        chip, core = me // 2, lax.rem(me, 2)
        self.me, self.chip, self.chips, self.core = me, chip, chips, core
        self.peer = 2 * chip + 1 - core
        self.plus = 2 * lax.rem(chip + 1, chips) + core
        self.minus = 2 * lax.rem(chip + chips - 1, chips) + core
        self.far = 2 * lax.rem(chip + 2, chips) + core
        self.seq_len = out.shape[1]
        self.piece = self.seq_len // SPLIT
        self.half = self.piece // 2

    def barrier(self, everyone):
        sem = pltpu.get_barrier_semaphore()
        count = lax.axis_size('model')
        near = (self.peer, self.plus, self.minus)
        devices = [lax.rem(self.me + r, count) for r in range(1, count)] if everyone else near
        for dev in devices:
            pl.semaphore_signal(sem, inc=1, device_id={'model': dev}, device_id_type=MESH)
        pl.semaphore_wait(sem, len(devices))

    def rcopy(self, h, kind, src, dst, dev):
        return pltpu.make_async_remote_copy(src_ref=src, dst_ref=dst, send_sem=self.send.at[h, kind],
                                            recv_sem=self.recv.at[h, kind], device_id={'model': dev}, device_id_type=MESH)

    def p(self, h): return pl.ds(h * self.piece, self.piece)
    def a(self, h): return pl.ds(h * self.piece, self.half)
    def b(self, h): return pl.ds(h * self.piece + self.half, self.half)

    def targets(self):
        return (self.far, self.plus, self.minus, self.me)

    def swap_copy(self, h, j):
        if self.give is not None:
            return self.rcopy(h, j, self.give.at[j, self.p(h)], self.swp.at[j, self.p(h)], self.peer)
        blk = self.targets()[j]
        other = blk + 1 - 2 * lax.rem(blk, 2)
        return self.rcopy(h, j, self.part.at[other, self.p(h)], self.swp.at[j, self.p(h)], self.peer)

    def produce_order(self, i):
        j, mine = i // 2, i % 2
        offset = 2 - j + 3 * (j // 2) + 2 * (j // 3)
        side = self.core * mine + (1 - self.core) * (1 - mine)
        return 2 * lax.rem(self.chip + offset, self.chips) + side

    def swap(self, j):
        for h in range(SPLIT):
            self.swap_copy(h, j).start()

    def load_copy(self, h, j):
        return pltpu.make_async_copy(self.part.at[self.targets()[j], self.p(h)], self.own.at[j, self.p(h)], self.load_sem.at[h, j])

    def c4(self, h): return self.rcopy(h, 4, self.own.at[0, self.a(h)], self.mid_a.at[h], self.plus)
    def c5(self, h): return self.rcopy(h, 5, self.own.at[0, self.b(h)], self.mid_b.at[h], self.minus)
    def c6(self, h): return self.rcopy(h, 6, self.own.at[1, self.b(h)], self.fin_p.at[self.b(h)], self.plus)
    def c7(self, h): return self.rcopy(h, 7, self.own.at[2, self.a(h)], self.fin_m.at[self.a(h)], self.minus)
    def c8(self, h): return self.rcopy(h, 8, self.own.at[1, self.a(h)], self.fin_p.at[self.a(h)], self.plus)
    def c9(self, h): return self.rcopy(h, 9, self.own.at[2, self.b(h)], self.fin_m.at[self.b(h)], self.minus)
    def c10(self, h): return self.rcopy(h, 10, self.rows.at[self.p(h)], self.out.at[self.me, self.p(h)], self.plus)
    def c11(self, h): return self.rcopy(h, 11, self.rows.at[self.p(h)], self.out.at[self.me, self.p(h)], self.minus)
    def c12(self, h): return self.rcopy(h, 12, self.rows.at[self.p(h)], self.out.at[self.me, self.p(h)], self.peer)
    def c13(self, h): return self.rcopy(h, 13, self.out.at[self.minus, self.a(h)], self.out.at[self.minus, self.a(h)], self.plus)
    def c14(self, h): return self.rcopy(h, 14, self.out.at[self.plus, self.b(h)], self.out.at[self.plus, self.b(h)], self.minus)
    def c15(self, h): return self.rcopy(h, 15, self.out.at[self.minus, self.p(h)], self.out.at[self.minus, self.p(h)], self.peer)
    def c16(self, h): return self.rcopy(h, 16, self.out.at[self.plus, self.p(h)], self.out.at[self.plus, self.p(h)], self.peer)
    def c17(self, h): return self.rcopy(h, 17, self.out.at[self.far, self.p(h)], self.out.at[self.far, self.p(h)], self.peer)
    def keep(self, h): return pltpu.make_async_copy(self.rows.at[self.p(h)], self.out.at[self.me, self.p(h)], self.store_sem.at[h])

    def begin(self, everyone=False):
        if self.give is not None:
            self.barrier(everyone)
            return
        for h in range(SPLIT):
            for j in range(4):
                self.load_copy(h, j).start()
        self.barrier(everyone)
        for h in range(SPLIT):
            for j in range(4):
                self.swap_copy(h, j).start()

    def add(self, j, row0, count, src, src_row0):
        def body(i, carry):
            at = pl.ds(pl.multiple_of(row0 + i * STEP, STEP), STEP)
            fr = pl.ds(pl.multiple_of(src_row0 + i * STEP, STEP), STEP)
            self.own[j, at] = (self.own[j, at].astype(jnp.float32) + src[fr].astype(jnp.float32)).astype(jnp.bfloat16)
            return carry
        lax.fori_loop(0, count // STEP, body, 0)

    def merge_swap(self, h, j):
        if self.give is None:
            self.load_copy(h, j).wait()
        self.swap_copy(h, j).wait_recv()
        self.add(j, h * self.piece, self.piece, self.swp.at[j], h * self.piece)

    def far_side(self, h):
        self.merge_swap(h, 0)
        self.c4(h).start()
        self.c5(h).start()

    def plus_direct(self, h):
        self.merge_swap(h, 1)
        self.c6(h).start()

    def minus_direct(self, h):
        self.merge_swap(h, 2)
        self.c7(h).start()

    def plus_sum(self, h):
        self.c4(h).wait_recv()
        self.add(1, h * self.piece, self.half, self.mid_a.at[h], 0)
        self.c8(h).start()

    def minus_sum(self, h):
        self.c5(h).wait_recv()
        self.add(2, h * self.piece + self.half, self.half, self.mid_b.at[h], 0)
        self.c9(h).start()

    def first(self, h):
        self.far_side(h)
        self.plus_direct(h)
        self.minus_direct(h)

    def second(self, h):
        self.plus_sum(h)
        self.minus_sum(h)

    def finish(self, h, middle):
        if self.give is None:
            self.load_copy(h, 3).wait()
        self.swap_copy(h, 3).wait_recv()
        self.c6(h).wait_recv()
        self.c8(h).wait_recv()
        self.c7(h).wait_recv()
        self.c9(h).wait_recv()

        def body(i, carry):
            at = pl.ds(pl.multiple_of(h * self.piece + i * STEP, STEP), STEP)
            f = lambda r: r.astype(jnp.float32)
            total = (f(self.own[3, at]) + f(self.swp[3, at])) + (f(self.fin_p[at]) + f(self.fin_m[at]))
            return middle(at, total, carry)
        return lax.fori_loop(0, self.piece // STEP, body, 0)

    def share(self, h):
        self.keep(h).start()
        self.c10(h).start()
        self.c11(h).start()
        self.c12(h).start()

    def forward(self, h):
        self.c10(h).wait_recv()
        self.c13(h).start()
        self.c15(h).start()
        self.c11(h).wait_recv()
        self.c14(h).start()
        self.c16(h).start()

    def last(self, h):
        self.c13(h).wait_recv()
        self.c14(h).wait_recv()
        self.c17(h).start()

    def end(self):
        for h in range(SPLIT):
            for c in (self.c12, self.c15, self.c16, self.c17):
                c(h).wait_recv()
            for j in range(4):
                self.swap_copy(h, j).wait_send()
            for c in (self.c4, self.c5, self.c6, self.c7, self.c8, self.c9, self.c10, self.c11, self.c12, self.c13, self.c14, self.c15, self.c16, self.c17):
                c(h).wait_send()
            self.keep(h).wait()


def ring_scratch(seq_len, hidden):
    bf = jnp.bfloat16
    return [pltpu.VMEM((4, seq_len, hidden), bf), pltpu.VMEM((4, seq_len, hidden), bf),
            pltpu.VMEM((SPLIT, seq_len // SPLIT // 2, hidden), bf), pltpu.VMEM((SPLIT, seq_len // SPLIT // 2, hidden), bf),
            pltpu.VMEM((seq_len, hidden), bf), pltpu.VMEM((seq_len, hidden), bf), pltpu.VMEM((seq_len, hidden), bf),
            pltpu.SemaphoreType.DMA((SPLIT, 4)), pltpu.SemaphoreType.DMA((SPLIT, KINDS)), pltpu.SemaphoreType.DMA((SPLIT, KINDS)),
            pltpu.SemaphoreType.DMA((SPLIT,))]


def any_spec():
    return pl.BlockSpec(memory_space=pl.ANY)


def dot_nn(lhs, rhs):
    return lax.dot_general(lhs, rhs, (((1,), (0,)), ((), ())), preferred_element_type=F32)


def dot_nt(lhs, rhs):
    return lax.dot_general(lhs, rhs, (((1,), (1,)), ((), ())), preferred_element_type=F32)


def dot_tn(lhs, rhs):
    return lax.dot_general(lhs, rhs, (((0,), (0,)), ((), ())), preferred_element_type=F32)


def norm_stats(values):
    mean_val = jnp.mean(values, axis=-1, keepdims=True)
    centered = values - mean_val
    var_val = jnp.mean(centered * centered, axis=-1, keepdims=True)
    return centered, lax.rsqrt(var_val + NORM_EPS)


def norm_back(values, gain, grad):
    centered, scale = norm_stats(values)
    unit = centered * scale
    d_unit = grad * gain
    mean_d = jnp.mean(d_unit, axis=-1, keepdims=True)
    mean_du = jnp.mean(d_unit * unit, axis=-1, keepdims=True)
    return scale * (d_unit - mean_d - unit * mean_du), grad * unit


def softmax_of(q, k, keep):
    scores = dot_nt(q, k) * (q.shape[-1] ** -0.5)
    scores = jnp.where(keep > 0.5, scores, -1e30)
    top = jnp.max(scores, axis=-1, keepdims=True)
    weights = jnp.exp(scores - top)
    return weights / jnp.sum(weights, axis=-1, keepdims=True)


def columns_dot(dot, out, lhs, rhs_of, width):
    for c in range(out.shape[-1] // width):
        out[:, c * width:(c + 1) * width] = dot(lhs, rhs_of(c * width, width)).astype(BF16)


def attention_seq(x, a, qkv, o, p1, keep, gain, wq, wo):
    def norm_step(i, carry):
        at = pl.ds(pl.multiple_of(i * NORM_STEP, NORM_STEP), NORM_STEP)
        centered, scale = norm_stats(x[at].astype(F32))
        a[at] = (centered * scale * gain[...].astype(F32)).astype(BF16)
        return carry
    lax.fori_loop(0, x.shape[0] // NORM_STEP, norm_step, 0)
    dim = 128
    for n in range(o.shape[-1] // dim):
        lo = 3 * n * dim
        qkv[:, lo:lo + 3 * dim] = dot_nn(a[...], wq[:, lo:lo + 3 * dim]).astype(BF16)
        q, k, v = (qkv[:, lo + j * dim:lo + (j + 1) * dim] for j in range(3))
        probs = softmax_of(q, k, keep[...]).astype(BF16)
        o[:, n * dim:(n + 1) * dim] = dot_nn(probs, v).astype(BF16)
    columns_dot(dot_nn, p1, o[...], lambda c, w: wo[:, c:c + w], 768)


def attention_back_seq(d_x1, qkv, keep, wq, wo, d_qkv, d_a):
    heads_width = wo.shape[0]
    dim = 128
    d_heads = dot_nt(d_x1[...], wo[...]).astype(BF16)
    for n in range(heads_width // dim):
        lo = 3 * n * dim
        q, k, v = (qkv[:, lo + j * dim:lo + (j + 1) * dim] for j in range(3))
        d_o = d_heads[:, n * dim:(n + 1) * dim]
        probs = softmax_of(q, k, keep[...])
        d_probs = dot_nt(d_o, v)
        row_dot = jnp.sum(d_probs * probs, axis=-1, keepdims=True)
        d_scores = (probs * (d_probs - row_dot) * (dim ** -0.5)).astype(BF16)
        d_qkv[:, lo:lo + dim] = dot_nn(d_scores, k).astype(BF16)
        d_qkv[:, lo + dim:lo + 2 * dim] = dot_tn(d_scores, q).astype(BF16)
        d_qkv[:, lo + 2 * dim:lo + 3 * dim] = dot_tn(probs.astype(BF16), d_o).astype(BF16)
    columns_dot(dot_nt, d_a, d_qkv[...], lambda c, w: wq[c:c + w, :], 512)


def load_wq(wq_hbm, wq, sems):
    dim = wq_hbm.shape[-1]
    return [pltpu.make_async_copy(wq_hbm.at[i], wq.at[:, pl.ds(i * dim, dim)], sems.at[i]) for i in range(wq_hbm.shape[0])]


class Once:
    def __init__(self, copies):
        self.copies = list(copies)

    def __call__(self):
        while self.copies:
            self.copies.pop().wait()


class Stream:
    def __init__(self, count, in_pairs, out_pairs, in_sem, out_sem):
        self.count, self.in_pairs, self.out_pairs, self.in_sem, self.out_sem = count, in_pairs, out_pairs, in_sem, out_sem

    def loads(self, i, slot):
        return [pltpu.make_async_copy(a, b, self.in_sem.at[k, slot]) for k, (a, b) in enumerate(self.in_pairs(i, slot))]

    def stores(self, i, slot):
        return [pltpu.make_async_copy(a, b, self.out_sem.at[k, slot]) for k, (a, b) in enumerate(self.out_pairs(i, slot))]

    def begin(self):
        for c in self.loads(0, 0):
            c.start()

    def run(self, lo, hi, body):
        def step(i, carry):
            slot = lax.rem(i, 2)
            for c in self.loads(i, slot):
                c.wait()

            @pl.when(i + 1 < self.count)
            def _():
                for c in self.loads(i + 1, 1 - slot):
                    c.start()

            @pl.when(i >= 2)
            def _():
                for c in self.stores(i - 2, slot):
                    c.wait()
            body(slot)
            for c in self.stores(i, slot):
                c.start()
            return carry
        lax.fori_loop(lo, hi, step, 0)

    def end(self):
        for i in (self.count - 2, self.count - 1):
            for c in self.stores(i, i % 2):
                c.wait()


def ring_params(cid):
    return pltpu.CompilerParams(collective_id=cid, has_side_effects=True, vmem_limit_bytes=VMEM_BYTES)


def sds(shape, dtype=BF16):
    return jax.ShapeDtypeStruct(shape, dtype)


def residual_events(ring, x_rows, x1_rows, gain, ready):
    def middle(at, total, carry):
        x1 = (x_rows[at].astype(F32) + total.astype(BF16).astype(F32)).astype(BF16)
        x1_rows[at] = x1
        centered, scale = norm_stats(x1.astype(F32))
        ring.rows[at] = (centered * scale * gain[...].astype(F32)).astype(BF16)
        return carry
    return ring_events(ring, middle, ready)


def ring_events(ring, middle, ready):
    events = []
    if ring.give is None:
        events += [functools.partial(ring.first, h) for h in range(SPLIT)]
        events += [functools.partial(ring.second, h) for h in range(SPLIT)]

    def close(h):
        ready()
        ring.finish(h, middle)
        ring.share(h)
    events += [functools.partial(close, h) for h in range(SPLIT)]
    events += [functools.partial(ring.forward, h) for h in range(SPLIT)]
    events += [functools.partial(ring.last, h) for h in range(SPLIT)]
    return events


def interleave(events, tasks, counts):
    pending = [[run, 0, total] for total, run in tasks]
    for event, n in zip(events, counts):
        while n and pending:
            run, lo, total = pending[0]
            hi = min(lo + n, total)
            run(lo, hi)
            n -= hi - lo
            pending[0][1] = hi
            if hi == total:
                pending.pop(0)
        event()
    for run, lo, total in pending:
        run(lo, total)


def ka_kernel(tokens, keep, gain_a, gain_m, wq_hbm, wo_hbm,
              b_out, x1_out, a_out, qkv_out, o_out, p1_out,
              x_rows, x1_rows, row_sem, wq, wo, wq_sem, wo_sem, x2, keep2, a2, qkv2, o2, p2, in_sem, out_sem,
              give, fx2, fkeep2, f_sem, *ring_scr):
    ring = Ring(None, b_out, *ring_scr, give=give)
    loads = [pltpu.make_async_copy(tokens.at[ring.me], x_rows, row_sem.at[0]), pltpu.make_async_copy(wo_hbm, wo, wo_sem)]
    weights = load_wq(wq_hbm, wq, wq_sem)
    again = Stream(tokens.shape[0], lambda i, t: [(tokens.at[i], x2.at[t]), (keep.at[i], keep2.at[t])],
                   lambda i, t: [(a2.at[t], a_out.at[i]), (qkv2.at[t], qkv_out.at[i]), (o2.at[t], o_out.at[i]), (p2.at[t], p1_out.at[i])],
                   in_sem, out_sem)
    once = Stream(tokens.shape[0], lambda i, t: [(tokens.at[ring.produce_order(i)], fx2.at[t]), (keep.at[ring.produce_order(i)], fkeep2.at[t])],
                  lambda i, t: [], f_sem, None)
    once.begin()
    for c in weights + loads:
        c.start()
    ring.begin()
    again.begin()
    ready = Once(weights + loads)
    ready()

    def task(lo, hi):
        again.run(lo, hi, lambda t: attention_seq(x2.at[t], a2.at[t], qkv2.at[t], o2.at[t], p2.at[t], keep2.at[t], gain_a, wq, wo))

    def produce(j):
        for mine, target in enumerate((give, ring.own)):
            once.run(2 * j + mine, 2 * j + mine + 1, lambda t: attention_seq(
                fx2.at[t], a2.at[t], qkv2.at[t], o2.at[t], target.at[j], fkeep2.at[t], gain_a, wq, wo))
            if not mine:
                ring.swap(j)
    pieces = range(SPLIT)
    produce(0)
    for h in pieces:
        ring.far_side(h)
    produce(1)
    for h in pieces:
        ring.plus_direct(h)
    for h in pieces:
        ring.plus_sum(h)
    produce(2)
    for h in pieces:
        ring.minus_direct(h)
    for h in pieces:
        ring.minus_sum(h)
    produce(3)
    interleave(residual_events(ring, x_rows, x1_rows, gain_m, ready), [(again.count, task)], KA_PLAN)
    keep_rows = pltpu.make_async_copy(x1_rows, x1_out, row_sem.at[1])
    keep_rows.start()
    again.end()
    keep_rows.wait()
    ring.end()


KA_PLAN = (1, 1, 2, 2, 2, 0)
PLAN = (0, 0, 1, 1, 2, 1, 2, 1, 0, 0)


def ka_call(tokens, keep, gain_a, gain_m, wq, wo, cid):
    seqs, seq_len, hidden = tokens.shape
    width, inner = wq.shape[0] * wq.shape[2], wo.shape[0]
    vm = pl.BlockSpec(memory_space=pltpu.VMEM)
    two = lambda w, t=BF16: pltpu.VMEM((2, seq_len, w), t)
    full = lambda w: sds((seqs, seq_len, w))
    return pl.pallas_call(
        ka_kernel, out_shape=(full(hidden), sds((seq_len, hidden)), full(hidden), full(width), full(inner), full(hidden)),
        in_specs=[any_spec()] * 2 + [vm, vm] + [any_spec()] * 2, out_specs=(any_spec(),) * 6,
        scratch_shapes=[pltpu.VMEM((seq_len, hidden), BF16), pltpu.VMEM((seq_len, hidden), BF16), pltpu.SemaphoreType.DMA((2,)),
                        pltpu.VMEM((hidden, width), BF16), pltpu.VMEM((inner, hidden), BF16), pltpu.SemaphoreType.DMA((wq.shape[0],)), pltpu.SemaphoreType.DMA,
                        two(hidden), two(seq_len, F32), two(hidden), two(width), two(inner), two(hidden),
                        pltpu.SemaphoreType.DMA((2, 2)), pltpu.SemaphoreType.DMA((4, 2)),
                        pltpu.VMEM((4, seq_len, hidden), BF16), two(hidden), two(seq_len, F32), pltpu.SemaphoreType.DMA((2, 2))] + ring_scratch(seq_len, hidden),
        compiler_params=ring_params(cid),
        cost_estimate=pl.CostEstimate(flops=80 * 10 ** 9, bytes_accessed=80 * 10 ** 6, transcendentals=0))(tokens, keep, gain_a, gain_m, wq, wo)


def gelu(values):
    return jax.nn.gelu(values, approximate=True)


def mlp_seq(b, d_out, p2, d_hid, hid, w_up, w_down):
    inner = w_up.shape[1]
    for c in range(0, inner, 256):
        hid[:, c:c + 256] = gelu(dot_nn(b[...], w_up[:, c:c + 256])).astype(BF16)
    columns_dot(dot_nn, p2, hid[...], lambda c, w: w_down[:, c:c + w], 512)
    columns_dot(dot_nt, d_hid, d_out[...], lambda c, w: w_down[c:c + w, :], 256)


def kb_kernel(p1, tokens, b_fwd, d_out, gain_m, up_hbm, down_hbm, b_out, x1_out, p2_out, dh_out,
              x_rows, x1_rows, row_sem, w_up, w_down, w_sem, b2, d2, p2, dh2, hid, in_sem, out_sem, *ring_scr):
    ring = Ring(p1, b_out, *ring_scr)
    ring.begin()
    loads = [pltpu.make_async_copy(tokens.at[ring.me], x_rows, row_sem.at[0]),
             pltpu.make_async_copy(up_hbm, w_up, w_sem.at[0]), pltpu.make_async_copy(down_hbm, w_down, w_sem.at[1])]
    stream = Stream(b_fwd.shape[0], lambda i, t: [(b_fwd.at[i], b2.at[t]), (d_out.at[i], d2.at[t])],
                    lambda i, t: [(p2.at[t], p2_out.at[i]), (dh2.at[t], dh_out.at[i])], in_sem, out_sem)
    for c in loads:
        c.start()
    stream.begin()
    ready = Once(loads)

    def task(lo, hi):
        ready()
        stream.run(lo, hi, lambda t: mlp_seq(b2.at[t], d2.at[t], p2.at[t], dh2.at[t], hid, w_up, w_down))
    interleave(residual_events(ring, x_rows, x1_rows, gain_m, ready), [(stream.count, task)], PLAN)
    keep_rows = pltpu.make_async_copy(x1_rows, x1_out, row_sem.at[1])
    keep_rows.start()
    stream.end()
    keep_rows.wait()
    ring.end()


def kb_call(p1, tokens, b_fwd, d_out, gain_m, w_up, w_down, cid):
    seqs, seq_len, hidden = tokens.shape
    inner = w_up.shape[1]
    vm = pl.BlockSpec(memory_space=pltpu.VMEM)
    return pl.pallas_call(
        kb_kernel, out_shape=(sds(tokens.shape), sds((seq_len, hidden)), sds(tokens.shape), sds((seqs, seq_len, inner))),
        in_specs=[any_spec()] * 4 + [vm] + [any_spec()] * 2, out_specs=(any_spec(),) * 4,
        scratch_shapes=[pltpu.VMEM((seq_len, hidden), BF16), pltpu.VMEM((seq_len, hidden), BF16), pltpu.SemaphoreType.DMA((2,)),
                        pltpu.VMEM((hidden, inner), BF16), pltpu.VMEM((inner, hidden), BF16), pltpu.SemaphoreType.DMA((2,)),
                        pltpu.VMEM((2, seq_len, hidden), BF16), pltpu.VMEM((2, seq_len, hidden), BF16), pltpu.VMEM((2, seq_len, hidden), BF16),
                        pltpu.VMEM((2, seq_len, inner), BF16), pltpu.VMEM((seq_len, inner), BF16),
                        pltpu.SemaphoreType.DMA((2, 2)), pltpu.SemaphoreType.DMA((2, 2))] + ring_scratch(seq_len, hidden),
        compiler_params=ring_params(cid),
        cost_estimate=pl.CostEstimate(flops=80 * 10 ** 9, bytes_accessed=80 * 10 ** 6, transcendentals=0))(p1, tokens, b_fwd, d_out, gain_m, w_up, w_down)


TILE = 384
NARROW = 128
GRAD_PLAN = (0, 0, 2, 4, 4, 2, 2, 2, 0, 0)


def wide_task(lhs_hbm, rhs, out_pairs, l2, g2, sems):
    in_sem, out_sem = sems
    stream = Stream(lhs_hbm.shape[1] // TILE, lambda i, t: [(lhs_hbm.at[:, pl.ds(pl.multiple_of(i * TILE, TILE), TILE)], l2.at[t])], out_pairs, in_sem, out_sem)

    def run(lo, hi):
        stream.run(lo, hi, lambda t: g2.__setitem__(t, dot_tn(l2[t], rhs[...]).astype(BF16)))
    return stream, run


def narrow_task(lhs_hbm, rhs, out_hbm, l2, g2, sems):
    in_sem, out_sem = sems
    span = lambda i: pl.ds(pl.multiple_of(i * NARROW, NARROW), NARROW)
    stream = Stream(lhs_hbm.shape[1] // NARROW, lambda i, t: [(lhs_hbm.at[:, span(i)], l2.at[t])], lambda i, t: [(g2.at[t], out_hbm.at[span(i)])], in_sem, out_sem)

    def run(lo, hi):
        def body(t):
            lhs = l2[t]
            for c in range(0, rhs.shape[1], 1024):
                g2[t, :, c:c + 1024] = dot_tn(lhs, rhs[:, c:c + 1024]).astype(BF16)
        stream.run(lo, hi, body)
    return stream, run


def after(ready, run):
    def call(lo, hi):
        ready()
        run(lo, hi)
    return call


def grad_kernel(last, part, values, resid, gain, wide_l, wide_r, narrow_l, narrow_r, *refs):
    if last:
        other_gain, out, gains_out, wide_out, narrow_out = refs[:5]
        refs = refs[5:]
    else:
        out, gain_out, wide_out, narrow_out = refs[:4]
        refs = refs[4:]
    v_rows, r_rows, row_sem, d_gain, w_r, w_l2, w_g2, n_r, n_l2, n_g2, rhs_sem, w_in, w_outs, n_in, n_outs = refs[:15]
    refs = refs[15:]
    if last:
        g_send, g_recv, g_ssem, g_rsem = refs[:4]
        refs = refs[4:]
    ring = Ring(part, out, *refs)
    ring.begin(everyone=last)
    loads = [pltpu.make_async_copy(values.at[ring.me] if len(values.shape) == 3 else values, v_rows, row_sem.at[0]),
             pltpu.make_async_copy(resid.at[ring.me], r_rows, row_sem.at[1]),
             pltpu.make_async_copy(wide_r, w_r, rhs_sem.at[0]), pltpu.make_async_copy(narrow_r, n_r, rhs_sem.at[1])]
    for c in loads:
        c.start()

    def wide_pairs(i, t):
        at = pl.ds(pl.multiple_of(i * TILE, TILE), TILE)
        if len(wide_out.shape) == 2:
            return [(w_g2.at[t], wide_out.at[at])]
        dim = wide_out.shape[2]
        return [(w_g2.at[t, :, pl.ds(j * dim, dim)], wide_out.at[j, at]) for j in range(wide_out.shape[0])]
    wide, wide_run = wide_task(wide_l, w_r, wide_pairs, w_l2, w_g2, (w_in, w_outs))
    narrow, narrow_run = narrow_task(narrow_l, n_r, narrow_out, n_l2, n_g2, (n_in, n_outs))
    wide.begin()
    narrow.begin()
    ready = Once(loads)

    d_gain[...] = jnp.zeros_like(d_gain)

    def middle(at, total, carry):
        d_value, d_gain_part = norm_back(v_rows[at].astype(F32), gain[...].astype(F32), total.astype(BF16).astype(F32))
        ring.rows[at] = (r_rows[at].astype(F32) + d_value).astype(BF16)
        d_gain[...] += d_gain_part
        return carry
    events = ring_events(ring, middle, ready)
    hidden = part.shape[2]
    count = lax.axis_size(AXIS)

    def gain_copy(r, sender):
        target = lax.rem(ring.me + r, count)
        return pltpu.make_async_remote_copy(src_ref=g_send, dst_ref=g_recv.at[sender], send_sem=g_ssem.at[r], recv_sem=g_rsem.at[sender],
                                            device_id={AXIS: target}, device_id_type=MESH)

    def gains():
        mine = jnp.sum(d_gain[...], axis=0, keepdims=True)
        if not last:
            gain_out[...] = mine
            return
        g_send[:, :hidden] = mine
        g_send[:, hidden:] = other_gain[...]
        g_recv[ring.me, :, :hidden] = mine
        g_recv[ring.me, :, hidden:] = other_gain[...]
        for r in range(1, count):
            gain_copy(r, ring.me).start()
    events.insert(2 * SPLIT + SPLIT, gains)
    plan = GRAD_PLAN[:3 * SPLIT] + (0,) + GRAD_PLAN[3 * SPLIT:]
    interleave(events, [(wide.count, after(ready, wide_run)), (narrow.count, after(ready, narrow_run))], plan)
    wide.end()
    narrow.end()
    ring.end()
    if last:
        for r in range(1, count):
            gain_copy(r, lax.rem(ring.me + r, count)).wait_recv()
            gain_copy(r, ring.me).wait_send()
        total = g_recv[0]
        for r in range(1, count):
            total = total + g_recv[r]
        gains_out[...] = total


def grad_call(part, values, resid, gain, wide_l, wide_r, narrow_l, narrow_r, blocks, cid, other_gain=None):
    seqs, seq_len, hidden = part.shape
    last = other_gain is not None
    vm = pl.BlockSpec(memory_space=pltpu.VMEM)
    rows, wide_n, narrow_n = wide_r.shape[0], wide_r.shape[1], narrow_r.shape[1]
    wide_shape = (wide_l.shape[1], wide_n) if blocks == 1 else (blocks, wide_l.shape[1], wide_n // blocks)
    dma = pltpu.SemaphoreType.DMA
    outs = (sds(part.shape), sds((1, 2 * hidden if last else hidden), F32), sds(wide_shape), sds((narrow_l.shape[1], narrow_n)))
    scratch = [pltpu.VMEM((seq_len, hidden), BF16), pltpu.VMEM((seq_len, hidden), BF16), dma((2,)), pltpu.VMEM((STEP, hidden), F32),
               pltpu.VMEM((rows, wide_n), BF16), pltpu.VMEM((2, rows, TILE), BF16), pltpu.VMEM((2, TILE, wide_n), BF16),
               pltpu.VMEM((rows, narrow_n), BF16), pltpu.VMEM((2, rows, NARROW), BF16), pltpu.VMEM((2, NARROW, narrow_n), BF16),
               dma((2,)), dma((1, 2)), dma((blocks, 2)), dma((1, 2)), dma((1, 2))]
    if last:
        count = lax.axis_size(AXIS)
        scratch += [pltpu.VMEM((1, 2 * hidden), F32), pltpu.VMEM((count, 1, 2 * hidden), F32), dma((count,)), dma((count,))]
    args = (part, values, resid, gain, wide_l, wide_r, narrow_l, narrow_r) + ((other_gain,) if last else ())
    return pl.pallas_call(
        functools.partial(grad_kernel, last), out_shape=outs,
        in_specs=[any_spec()] * 3 + [vm] + [any_spec()] * 4 + ([vm] if last else []), out_specs=(any_spec(), vm, any_spec(), any_spec()),
        scratch_shapes=scratch + ring_scratch(seq_len, hidden), compiler_params=ring_params(cid),
        cost_estimate=pl.CostEstimate(flops=80 * 10 ** 9, bytes_accessed=80 * 10 ** 6, transcendentals=0))(*args)


def back_kernel(d_x1, qkv, keep, wq_hbm, wo, g_up, g_down, d_qkv, d_a, up_out, down_out, wq, sems):
    up_out[...] = g_up[...]
    down_out[...] = g_down[...]

    @pl.when(pl.program_id(0) == 0)
    def _():
        copies = load_wq(wq_hbm, wq, sems)
        for c in copies:
            c.start()
        for c in copies:
            c.wait()
    attention_back_seq(d_x1.at[0], qkv.at[0], keep.at[0], wq, wo, d_qkv.at[0], d_a.at[0])


def back_call(d_x1, qkv, keep, wq, wo, g_up, g_down):
    seqs, seq_len, hidden = d_x1.shape
    width = qkv.shape[-1]
    part = lambda g: pl.BlockSpec((g.shape[0] // seqs, g.shape[1]), lambda i: (i, 0))
    seq = lambda w: pl.BlockSpec((1, seq_len, w), lambda i: (i, 0, 0))
    return pl.pallas_call(
        back_kernel, grid=(seqs,), out_shape=(sds(qkv.shape), sds(d_x1.shape), sds(g_up.shape), sds(g_down.shape)),
        in_specs=[seq(hidden), seq(width), seq(seq_len), any_spec(), pl.BlockSpec(wo.shape, lambda i: (0, 0)), part(g_up), part(g_down)],
        out_specs=(seq(width), seq(hidden), part(g_up), part(g_down)),
        scratch_shapes=[pltpu.VMEM((hidden, width), BF16), pltpu.SemaphoreType.DMA((wq.shape[0],))],
        compiler_params=pltpu.CompilerParams(vmem_limit_bytes=VMEM_BYTES),
        cost_estimate=pl.CostEstimate(flops=20 * 10 ** 9, bytes_accessed=30 * 10 ** 6, transcendentals=0))(d_x1, qkv, keep, wq, wo, g_up, g_down)


def put_kernel(*refs):
    half = len(refs) // 2
    for source, target in zip(refs[:half], refs[half:]):
        target[...] = source[...]


def put_call(*arrays):
    steps = 8

    def spec(v):
        axis = max(range(v.ndim - 1), key=lambda k: v.shape[k])
        shape = tuple(n // steps if k == axis else n for k, n in enumerate(v.shape))
        return pl.BlockSpec(shape, lambda i: tuple(i if k == axis else 0 for k in range(v.ndim)))
    specs = [spec(v) for v in arrays]
    return pl.pallas_call(put_kernel, grid=(steps,), out_shape=tuple(sds(v.shape, v.dtype) for v in arrays), in_specs=specs, out_specs=tuple(specs),
                          compiler_params=pltpu.CompilerParams(vmem_limit_bytes=VMEM_BYTES),
                          cost_estimate=pl.CostEstimate(flops=10 ** 6, bytes_accessed=60 * 10 ** 6, transcendentals=0))(*arrays)


def dot_of(spec, lhs, rhs):
    return jnp.einsum(spec, lhs, rhs, preferred_element_type=F32)


def solution(mesh):
    def device_step(tokens, seg_ids, d_out, gain_attn, gain_mlp, w_qkv, w_out, w_up, w_down):
        seqs, seq_len, hidden = tokens.shape
        row_count = seqs * seq_len
        heads, dim = w_qkv.shape[1], w_qkv.shape[3]
        at_pos = lax.broadcasted_iota(jnp.int32, (seq_len, seq_len), 0) >= lax.broadcasted_iota(jnp.int32, (seq_len, seq_len), 1)
        keep = ((seg_ids[:, :, None] == seg_ids[:, None, :]) & at_pos[None]).astype(F32)
        gain_a, gain_m = gain_attn[None], gain_mlp[None]
        wq = jnp.transpose(w_qkv, (1, 2, 0, 3)).reshape(heads * 3, hidden, dim)
        wo = w_out.reshape(heads * dim, hidden)
        flat = lambda v: v.reshape(row_count, v.shape[-1])

        b_full, x1_rows, normed, qkv, heads_out, p1_again = ka_call(tokens, keep, gain_a, gain_m, wq, wo, 0)
        b_again, x1_again, p2, d_hidden = kb_call(p1_again, tokens, b_full, d_out, gain_m, w_up, w_down, 1)
        p2_rows = lax.psum_scatter(flat(p2), AXIS, scatter_dimension=0, tiled=True)
        out_rows = (x1_rows.astype(F32) + p2_rows.astype(F32)).astype(BF16)

        pre_act = dot_of('rh,hf->rf', flat(b_again), w_up)
        hidden_act, gelu_back = jax.vjp(gelu, pre_act)
        hidden_act = hidden_act.astype(BF16)
        d_pre = gelu_back(flat(d_hidden).astype(F32))[0].astype(BF16)
        d_b = dot_of('rf,hf->rh', d_pre, w_up).astype(BF16).reshape(tokens.shape)
        d_x1, d_gain_m, d_w_up, d_w_down = grad_call(d_b, x1_again, d_out, gain_m, flat(b_again), d_pre, hidden_act, flat(d_out), 1, 2)
        d_x1, out_rows = lax.optimization_barrier((d_x1, out_rows))
        layer_out = lax.all_gather(out_rows, AXIS, axis=0, tiled=True).reshape(tokens.shape)
        d_qkv, d_a, d_w_up, d_w_down = back_call(d_x1, qkv, keep, wq, wo, d_w_up, d_w_down)
        d_tokens, d_gain, d_wq, d_wo = grad_call(d_a, tokens, d_x1, gain_a, flat(normed), flat(d_qkv), flat(heads_out), flat(d_x1), heads * 3, 3, d_gain_m)
        layer_out, d_tokens, d_wq, d_wo = put_call(layer_out, d_tokens, d_wq, d_wo)
        d_w_qkv = jnp.transpose(d_wq.reshape(heads, 3, hidden, dim), (2, 0, 1, 3))
        d_w_out = d_wo.reshape(w_out.shape)
        d_gain_a, d_gain_m = d_gain[0, :hidden], d_gain[0, hidden:]
        return layer_out, d_tokens, d_w_qkv, d_w_out, d_w_up, d_w_down, d_gain_a, d_gain_m

    in_specs = (P('data', None, None), P('data', None), P('data', None, None), P(), P(), P(None, 'model', None, None), P('model', None, None), P(None, 'model'), P('model', None))
    out_specs = (P('data', None, None), P('data', None, None), P('data', 'model', None, None), P(('data', 'model'), None, None), P('data', 'model'), P(('data', 'model'), None), P('data'), P('data'))
    return jax.shard_map(device_step, mesh=mesh, in_specs=in_specs, out_specs=out_specs, check_vma=False)
```
